32 devices in a mesh: dp: 8 (over z, y), tensor: 4 (over x, core).
Axes of the slice: x: 2, y: 2, z: 4, core: 2. Of those that a mesh axis runs over, the one named last changes fastest.
Arguments:
- layer_outs: bfloat16 [5, 8192, 4096], P(None, 'dp', 'tensor'), may hold values from -6 to 6
- avg_grads: bfloat16 [4, 8192, 4096], P(None, 'dp', 'tensor'), may hold values from -0.0010299683 to 0.0010299683
- attn_mixed: bfloat16 [8192, 4096], P('dp', 'tensor'), may hold values from -96 to 96
- dwa_coefs: float32 [4, 5], replicated, may hold values from -1.5 to 1.5
Outputs:
- coef_grad: float32 [4, 5], replicated
- proj_grad: float32 [4096, 4096], P('dp', 'tensor')
The draws below stay inside these ranges and needn't reach their ends.
All inputs are finite; a program needn't handle non-finite values.
Results may differ from the reference program's by a relative error of at most 0.0042.
Values may be sent and summed in bfloat16 or wider, within the bound.
No kernel may reach another device: no remote copies, remote signals or barrier semaphores. Data moves between devices by JAX's collectives and lax.ppermute only.
A program may use at most 128 MiB of HBM per device.

```python
import jax
import jax.numpy as jnp
from jax import lax

D = 4096
LAYERS = 4
TOKENS = 8192


def steps_of(rng, dims, split, least, largest):
    factor_of, own = 1.0, jax.random.fold_in(rng, 6)
    for dim, blocks in split:
        heights = jnp.exp(jax.random.uniform(jax.random.fold_in(own, dim), (blocks,), jnp.float32, least / len(split), largest / len(split)))
        factor_of = factor_of * jnp.repeat(heights, dims[dim] // blocks).reshape([-1 if axis == dim else 1 for axis in range(len(dims))])
    return factor_of


def bell_draw(own_key, dims, scale, bound, split=(), kind=jnp.bfloat16):
    array = scale * jax.random.normal(own_key, dims, jnp.float32)
    if split:
        array = array * steps_of(own_key, dims, split, -0.22, 0.18)
    return jnp.clip(array, -bound, bound).astype(kind)


def setup_inputs(seed: int = 0) -> dict:
    keys = jax.random.split(jax.random.key(seed), 5)
    layer_outs = bell_draw(keys[0], (LAYERS + 1, TOKENS, D), 1.0, 6.0, ((1, 8), (2, 4)))
    avg_grads = bell_draw(keys[1], (LAYERS, TOKENS, D), (1.0 / (TOKENS * D) ** 0.5), 0.0010299683, ((1, 8), (2, 4)))
    attn_mixed = bell_draw(keys[2], (TOKENS, D), (D ** 0.5 / 4), 96.0, ((0, 8), (1, 4)))
    dwa_coefs = jnp.clip(jax.random.uniform(keys[3], (LAYERS, LAYERS + 1), jnp.float32, -1.5, 1.5), -1.5, 1.5)
    return dict(layer_outs=layer_outs, avg_grads=avg_grads, attn_mixed=attn_mixed, dwa_coefs=dwa_coefs)


def reference(layer_outs, avg_grads, attn_mixed, dwa_coefs):
    grads_flat = avg_grads.reshape(LAYERS, -1)
    outs_flat = layer_outs.reshape(LAYERS + 1, -1)
    raw = lax.dot_general(grads_flat, outs_flat, (((1,), (1,)), ((), ())), preferred_element_type=jnp.float32)
    rows = jnp.arange(LAYERS, dtype=jnp.int32)[:, None]
    cols = jnp.arange(LAYERS + 1, dtype=jnp.int32)[None, :]
    coef_grad = jnp.where(cols <= rows + 1, raw, jnp.float32(0.0))
    first = dwa_coefs[LAYERS - 2, LAYERS - 1] * avg_grads[LAYERS - 2].astype(jnp.float32)
    second = dwa_coefs[LAYERS - 1, LAYERS - 1] * avg_grads[LAYERS - 1].astype(jnp.float32)
    out_grad = (first + second).astype(jnp.bfloat16)
    proj_grad = lax.dot_general(out_grad, attn_mixed, (((0,), (0,)), ((), ())), preferred_element_type=jnp.float32)
    return coef_grad, proj_grad
```

```python
import jax
import jax.numpy as jnp
from jax import lax
from jax.experimental import pallas as pl
from jax.experimental.pallas import tpu as pltpu
from jax.sharding import PartitionSpec as P

CHUNKS = 4
ROWS = 128
SUB = 16
LANES = 128


def coef_kernel(outs_ref, grads_ref, sums_ref):
    depth, rows, width = grads_ref.shape
    pairs = [(i, j) for i in range(depth) for j in range(min(i + 2, depth + 1))]

    @pl.when(pl.program_id(0) == 0)
    def _():
        sums_ref[...] = jnp.zeros_like(sums_ref)

    def step(r, sums):
        start = pl.multiple_of(r * SUB, SUB)
        for c in range(width // LANES):
            cols = pl.ds(c * LANES, LANES)
            outs = [outs_ref[j, pl.ds(start, SUB), cols].astype(jnp.float32) for j in range(depth + 1)]
            grads = [grads_ref[i, pl.ds(start, SUB), cols].astype(jnp.float32) for i in range(depth)]
            sums = tuple(s + grads[i] * outs[j] for s, (i, j) in zip(sums, pairs))
        return sums

    zero = jnp.zeros((SUB, LANES), jnp.float32)
    sums = lax.fori_loop(0, rows // SUB, step, tuple(zero for _ in pairs))
    for s, (i, j) in zip(sums, pairs):
        sums_ref[i, j] += s


def coef_partial(layer_outs, avg_grads):
    depth, tokens, width = avg_grads.shape
    shape = (depth, depth + 1, SUB, LANES)
    sums = pl.pallas_call(
        coef_kernel,
        grid=(tokens // ROWS,),
        in_specs=[
            pl.BlockSpec((depth + 1, ROWS, width), lambda b: (0, b, 0)),
            pl.BlockSpec((depth, ROWS, width), lambda b: (0, b, 0)),
        ],
        out_specs=pl.BlockSpec(shape, lambda b: (0, 0, 0, 0)),
        out_shape=jax.ShapeDtypeStruct(shape, jnp.float32),
        compiler_params=pltpu.CompilerParams(dimension_semantics=("arbitrary",)),
        cost_estimate=pl.CostEstimate(
            flops=40 * depth * (depth + 1) * tokens * width,
            bytes_accessed=2 * (2 * depth + 1) * tokens * width,
            transcendentals=0,
        ),
        name="coef_sums",
    )(layer_outs, avg_grads)
    return jnp.sum(sums, axis=(2, 3))


def weight_grad(avg_grads, attn_mixed, dwa_coefs):
    depth, tokens, width = avg_grads.shape
    dp, tensor = lax.axis_size("dp"), lax.axis_size("tensor")
    near = dp // tensor
    far = dp // near
    rows = width * tensor // dp
    cores = 2
    chips = tensor // cores
    place = lax.axis_index("dp")
    far_at, near_at = place // near, place % near
    mine = lax.axis_index("tensor")
    chip_at, core_at = mine // cores, mine % cores

    def near_shift(value, by):
        return lax.ppermute(value, "dp", [(d, d // near * near + (d % near + by) % near) for d in range(dp)])

    def far_shift(value, by):
        return lax.ppermute(value, "dp", [(d, (d // near + by) % far * near + d % near) for d in range(dp)])

    def core_swap(value):
        return lax.ppermute(value, "tensor", [(t, t // cores * cores + (t % cores + 1) % cores) for t in range(tensor)])

    def chip_fetch(value, by):
        return lax.ppermute(value, "tensor", [(t, (t // cores - by) % chips * cores + t % cores) for t in range(tensor)])

    def out_grad(at):
        def part(i):
            return lax.dynamic_slice(avg_grads, (i, 0, at * rows), (1, tokens, rows))[0].astype(jnp.float32)

        first = dwa_coefs[depth - 2, depth - 1] * part(depth - 2)
        second = dwa_coefs[depth - 1, depth - 1] * part(depth - 1)
        return (first + second).astype(jnp.bfloat16)

    grads = [out_grad(near_at)]
    for by in range(1, near):
        grads.append(near_shift(out_grad((near_at + by) % near), by))

    chunk = attn_mixed.shape[1] // CHUNKS
    own = [attn_mixed[:, c * chunk : (c + 1) * chunk] for c in range(CHUNKS)]
    sent, _ = lax.optimization_barrier((own, grads))
    mixed = [[o] + [near_shift(s, by) for by in range(1, near)] for o, s in zip(own, sent)]

    gathered = []
    for piece in grads:
        blocks = []
        for by in range(chips):
            block = piece if by == 0 else chip_fetch(piece, by)
            blocks += [block, core_swap(block)]
        gathered.append(jnp.stack(blocks))

    def grads_for(hop):
        to = (far_at + hop) % far
        at = (to // cores - chip_at) % chips * cores + (to % cores - core_at) % cores
        return [lax.dynamic_index_in_dim(g, at, 0, keepdims=False) for g in gathered]

    ordered = [grads_for(hop) for hop in range(far)]

    def product(hop, c):
        total = None
        for g, m in zip(ordered[hop % far], mixed[c]):
            term = lax.dot_general(g, m, (((0,), (0,)), ((), ())), preferred_element_type=jnp.float32)
            total = term if total is None else total + term
        return total

    outs = []
    for c in range(CHUNKS):
        total = product(0, c)
        up = far // 2 if c % 2 == 0 else (far - 1) // 2
        for sign, length in ((1, up), (-1, far - 1 - up)):
            carried = None
            for hop in range(length, 0, -1):
                term = product(sign * hop, c)
                if carried is not None:
                    term = term + carried.astype(jnp.float32)
                carried = far_shift(term.astype(jnp.bfloat16), sign)
            if carried is not None:
                total = total + carried.astype(jnp.float32)
        outs.append(total)
    return jnp.concatenate(outs, axis=1), mixed[max(CHUNKS - 2, 0)]


def total_over(value, axis):
    size = lax.axis_size(axis)
    if size & (size - 1):
        return lax.psum(value, axis)
    step = 1
    while step < size:
        value = value + lax.ppermute(value, axis, [(d, d ^ step) for d in range(size)])
        step *= 2
    return value


def local(layer_outs, avg_grads, attn_mixed, dwa_coefs):
    proj_grad, arrived = weight_grad(avg_grads, attn_mixed, dwa_coefs)
    partial_sum, _ = lax.optimization_barrier((coef_partial(layer_outs, avg_grads), arrived))
    raw = total_over(total_over(partial_sum, "tensor"), "dp")
    return (raw, proj_grad)


def solution(mesh):
    in_specs = (P(None, "dp", "tensor"), P(None, "dp", "tensor"), P("dp", "tensor"), P())
    out_specs = (P(), P("dp", "tensor"))
    return jax.shard_map(local, mesh=mesh, in_specs=in_specs, out_specs=out_specs, check_vma=False)
```

```python
import jax
import jax.numpy as jnp
from jax import lax
from jax.experimental import pallas as pl
from jax.experimental.pallas import tpu as pltpu
from jax.sharding import PartitionSpec as P


CHUNKS = 4
ROWS = 128
SUB = 16
LANES = 128


def coef_kernel(outs_ref, grads_ref, sums_ref):
    depth, rows, width = grads_ref.shape
    pairs = [(i, j) for i in range(depth) for j in range(min(i + 2, depth + 1))]

    @pl.when(pl.program_id(0) == 0)
    def _():
        sums_ref[...] = jnp.zeros_like(sums_ref)

    def step(r, sums):
        start = pl.multiple_of(r * SUB, SUB)
        for c in range(width // LANES):
            cols = pl.ds(c * LANES, LANES)
            outs = [outs_ref[j, pl.ds(start, SUB), cols].astype(jnp.float32) for j in range(depth + 1)]
            grads = [grads_ref[i, pl.ds(start, SUB), cols].astype(jnp.float32) for i in range(depth)]
            sums = tuple(s + grads[i] * outs[j] for s, (i, j) in zip(sums, pairs))
        return sums

    zero = jnp.zeros((SUB, LANES), jnp.float32)
    sums = lax.fori_loop(0, rows // SUB, step, tuple(zero for _ in pairs))
    for s, (i, j) in zip(sums, pairs):
        sums_ref[i, j] += s


def coef_partial(layer_outs, avg_grads):
    depth, tokens, width = avg_grads.shape
    shape = (depth, depth + 1, SUB, LANES)
    sums = pl.pallas_call(
        coef_kernel,
        grid=(tokens // ROWS,),
        in_specs=[
            pl.BlockSpec((depth + 1, ROWS, width), lambda b: (0, b, 0)),
            pl.BlockSpec((depth, ROWS, width), lambda b: (0, b, 0)),
        ],
        out_specs=pl.BlockSpec(shape, lambda b: (0, 0, 0, 0)),
        out_shape=jax.ShapeDtypeStruct(shape, jnp.float32),
        compiler_params=pltpu.CompilerParams(dimension_semantics=("arbitrary",)),
        cost_estimate=pl.CostEstimate(
            flops=40 * depth * (depth + 1) * tokens * width,
            bytes_accessed=2 * (2 * depth + 1) * tokens * width,
            transcendentals=0,
        ),
        name="coef_sums",
    )(layer_outs, avg_grads)
    return jnp.sum(sums, axis=(2, 3))


def weight_grad(avg_grads, attn_mixed, dwa_coefs):
    depth, tokens, width = avg_grads.shape
    dp, tensor = lax.axis_size("dp"), lax.axis_size("tensor")
    near = dp // tensor
    far = dp // near
    rows = width * tensor // dp
    cores = 2
    chips = tensor // cores
    place = lax.axis_index("dp")
    far_at, near_at = place // near, place % near
    mine = lax.axis_index("tensor")
    chip_at, core_at = mine // cores, mine % cores

    def near_shift(value, by):
        return lax.ppermute(value, "dp", [(d, d // near * near + (d % near + by) % near) for d in range(dp)])

    def far_shift(value, by):
        return lax.ppermute(value, "dp", [(d, (d // near + by) % far * near + d % near) for d in range(dp)])

    def core_swap(value):
        return lax.ppermute(value, "tensor", [(t, t // cores * cores + (t % cores + 1) % cores) for t in range(tensor)])

    def chip_fetch(value, by):
        return lax.ppermute(value, "tensor", [(t, (t // cores - by) % chips * cores + t % cores) for t in range(tensor)])

    def out_grad(at):
        def part(i):
            return lax.dynamic_slice(avg_grads, (i, 0, at * rows), (1, tokens, rows))[0].astype(jnp.float32)

        first = dwa_coefs[depth - 2, depth - 1] * part(depth - 2)
        second = dwa_coefs[depth - 1, depth - 1] * part(depth - 1)
        return (first + second).astype(jnp.bfloat16)

    grads = [out_grad(near_at)]
    for by in range(1, near):
        piece = out_grad((near_at + by) % near)
        grads.append(near_shift(piece, by))

    chunk = attn_mixed.shape[1] // CHUNKS
    own = [attn_mixed[:, c * chunk : (c + 1) * chunk] for c in range(CHUNKS)]
    sent, _ = lax.optimization_barrier((own, grads))
    mixed = []
    for c in range(CHUNKS):
        mixed.append([own[c]] + [near_shift(sent[c], by) for by in range(1, near)])

    gathered = []
    for piece in grads:
        blocks = []
        for by in range(chips):
            block = piece if by == 0 else chip_fetch(piece, by)
            blocks += [block, core_swap(block)]
        gathered.append(jnp.stack(blocks))
        gathered_last = blocks[-2]

    def grads_for(hop):
        to = (far_at + hop) % far
        at = (to // cores - chip_at) % chips * cores + (to % cores - core_at) % cores
        return [lax.dynamic_index_in_dim(g, at, 0, keepdims=False) for g in gathered]

    ordered = [grads_for(hop) for hop in range(far)]

    def product(hop, c):
        total = None
        for g, m in zip(ordered[hop % far], mixed[c]):
            term = lax.dot_general(g, m, (((0,), (0,)), ((), ())), preferred_element_type=jnp.float32)
            total = term if total is None else total + term
        return total

    outs = []
    for c in range(CHUNKS):
        total = product(0, c)
        up = far // 2 if c % 2 == 0 else (far - 1) // 2
        for sign, length in ((1, up), (-1, far - 1 - up)):
            carried = None
            for hop in range(length, 0, -1):
                term = product(sign * hop, c)
                if carried is not None:
                    term = term + carried.astype(jnp.float32)
                carried = far_shift(term.astype(jnp.bfloat16), sign)
            if carried is not None:
                total = total + carried.astype(jnp.float32)
        outs.append(total)
    return jnp.concatenate(outs, axis=1), (gathered_last, mixed[-1])


def exchanged(value, axis, begin, end):
    size = lax.axis_size(axis)
    while begin < end:
        value = value + lax.ppermute(value, axis, [(d, d ^ begin) for d in range(size)])
        begin *= 2
    return value


def after(value, gate):
    return lax.optimization_barrier((value, gate))[0]


def local(layer_outs, avg_grads, attn_mixed, dwa_coefs):
    partial_sum = coef_partial(layer_outs, avg_grads)
    proj_grad, (fetched, mixed) = weight_grad(avg_grads, attn_mixed, dwa_coefs)
    dp, tensor = lax.axis_size("dp"), lax.axis_size("tensor")
    near = dp // tensor
    raw = exchanged(partial_sum, "tensor", 1, 2)
    raw = exchanged(raw, "dp", near, dp)
    raw = exchanged(after(raw, (fetched, mixed)), "tensor", 2, tensor)
    raw = exchanged(raw, "dp", 1, near)
    return (raw, proj_grad)


def solution(mesh):
    in_specs = (P(None, "dp", "tensor"), P(None, "dp", "tensor"), P("dp", "tensor"), P())
    out_specs = (P(), P("dp", "tensor"))
    return jax.shard_map(local, mesh=mesh, in_specs=in_specs, out_specs=out_specs, check_vma=False)
```
